32 devices in a mesh: dom: 16 (over z, y, core), sub: 2 (over x).
Axes of the slice: x: 2, y: 2, z: 4, core: 2. Of those that a mesh axis runs over, the one named last changes fastest.
Arguments:
- solution: float32 [125, 5, 1024], P(None, None, ('dom', 'sub')), may hold values from -1.2 to 5.4, as said below
- face_link: int32 [6, 1024], P(None, ('dom', 'sub')), may hold values from 0 to 6143, as said below
Outputs:
- rate: float32 [125, 5, 1024], P(None, None, ('dom', 'sub'))
The draws below stay inside these ranges and needn't reach their ends.
Inputs may be any that keep to these rules, and one draw needn't show every extreme that they name: At every solution point density lies between 0.6 and 1.4, each velocity component between -0.8 and 0.8 and pressure between 0.6 and 1.6; at every flux point the interpolated density and pressure stay at 0.5 or more and each interpolated velocity component between -1.1 and 1.1. `face_link`: the pairing is mutual and pairs face 2 a + 1 of one element with face 2 a of another, point for point. Elements are numbered device by device in the order of the joined axes, 32 to a device; a partner lies in the same partition or in one whose dom index differs by at most 2 cyclically. At most 6 faces of one device pair with faces of any one other device, and in every draw some pair of devices reaches 6.
All inputs are finite; a program needn't handle non-finite values.
Results may differ from the reference program's by a relative error of at most 0.0003.
Values sent between devices are 32-bit elements; how exact they have to be, the bound alone decides.
A program may use at most 64 MiB of HBM per device.

```python
import jax
import jax.numpy as jnp
import numpy as np
from jax import lax

ORDER = 4
NSIDE = 5
NPTS = 125
ELEM_DEV = 32
CAP = 6
ELEMS = 1024
N_DOM = 16
N_SUB = 2


heat_ratio = 1.4


def point_coordinates():
    point_ids = jnp.arange(NPTS, dtype=jnp.int32)
    index_list = [point_ids // (NSIDE * NSIDE), point_ids // NSIDE % NSIDE, point_ids % NSIDE]
    half_span = 0.5 * (NSIDE - 1)
    return jnp.stack([(member.astype(jnp.float32) - half_span) / half_span for member in index_list])


def smooth_field(key, count, mean_lo, mean_hi, slope_amp, noise_amp):
    key_mean, key_slope, key_noise = jax.random.split(key, 3)
    coords = point_coordinates()
    means = jax.random.uniform(key_mean, (count, 1, ELEMS), jnp.float32, mean_lo, mean_hi)
    slopes = jax.random.uniform(key_slope, (count, 3, ELEMS), jnp.float32, -slope_amp, slope_amp)
    linear = jnp.einsum('cae,ap->cpe', slopes, coords)
    noise = jax.random.uniform(key_noise, (count, NPTS, ELEMS), jnp.float32, -noise_amp, noise_amp)
    return means + linear + noise


def draw_solution(key, part):
    subkeys = jax.random.split(key, 3)
    density = smooth_field(subkeys[0], 1, 0.9, 1.1, 0.03, 0.04)[0]
    mean_flow = jnp.array([0.2, 0.0, -0.1], jnp.float32).reshape(3, 1, 1)
    velocity = mean_flow + smooth_field(subkeys[1], 3, -0.2, 0.2, 0.05, 0.08)
    pressure = smooth_field(subkeys[2], 1, 0.9, 1.1, 0.03, 0.04)[0]
    energy = pressure / (heat_ratio - 1.0) + 0.5 * density * jnp.sum(velocity * velocity, axis=0)
    momentum = density[None] * velocity
    return jnp.stack([density, momentum[0], momentum[1], momentum[2], energy], axis=1).astype(jnp.float32)


def draw_face_link(key, part):
    devices = N_DOM * N_SUB
    dev_ids = jnp.arange(devices, dtype=jnp.int32)
    dom_ids = dev_ids // N_SUB
    sub_ids = dev_ids % N_SUB
    classes = jnp.arange(N_SUB, dtype=jnp.int32)
    slots = jnp.arange(ELEM_DEV, dtype=jnp.int32)
    pick_pair, pick_far = jax.random.split(jax.random.fold_in(key, 101))
    star_pair = jax.random.randint(pick_pair, (), 1, N_SUB)
    star_far = jax.random.randint(pick_far, (), 0, N_SUB)
    ceilings = (CAP - 2 * (CAP // 3), CAP // 3, CAP // 3)
    link_table = jnp.zeros((6, devices, ELEM_DEV), jnp.int32)
    for direction in range(3):
        ceiling = ceilings[direction]
        half_cap = ceiling // 2
        key_pair, key_far, key_near, key_slot, key_elem = jax.random.split(jax.random.fold_in(key, direction), 5)
        pairs = jax.random.randint(key_pair, (N_SUB,), 0, half_cap + 1)
        pairs = jnp.where((classes == star_pair) | (classes == (N_SUB - star_pair) % N_SUB), half_cap, pairs)
        pairs = jnp.where(classes == 0, 0, pairs)
        remote = jax.random.randint(key_far, (N_SUB,), ceiling, 2 * ceiling + 1)
        remote = jnp.where(classes == star_far, 2 * ceiling, remote)
        block_sizes = jnp.concatenate([pairs, remote])
        block_ends = jnp.cumsum(block_sizes)
        block_starts = block_ends - block_sizes
        block_of = jnp.sum((slots[:, None] >= block_ends[None, :]).astype(jnp.int32), axis=1)
        inside = block_of < 2 * N_SUB
        clamped = jnp.minimum(block_of, 2 * N_SUB - 1)
        shift_sub = jnp.where(inside, clamped % N_SUB, 0)
        offset_in = slots - block_starts[clamped]
        near_count = jax.random.randint(key_near, (N_SUB, N_SUB), remote[None, :] - ceiling, ceiling + 1)
        far_block = inside & (block_of >= N_SUB)
        near_at = near_count[:, shift_sub]
        hops = jnp.where(far_block[None, :], jnp.where(offset_in[None, :] < near_at, 1, 2), 0)
        reorder = jax.random.permutation(key_slot, ELEM_DEV)
        shift_sub = shift_sub[reorder]
        hops = hops[:, reorder]
        members = jax.vmap(lambda elem_key: jax.random.permutation(elem_key, ELEM_DEV))(jax.random.split(key_elem, devices)).astype(jnp.int32)
        dest_dom = (dom_ids[:, None] + hops[sub_ids]) % N_DOM
        dest_sub = (sub_ids[:, None] + shift_sub[None, :]) % N_SUB
        dest_dev = dest_dom * N_SUB + dest_sub
        dest_elem = members[dest_dev, slots[None, :]]
        own_global = dev_ids[:, None] * ELEM_DEV + members
        dest_global = dest_dev * ELEM_DEV + dest_elem
        link_table = link_table.at[2 * direction + 1, dev_ids[:, None], members].set(dest_global * 6 + 2 * direction)
        link_table = link_table.at[2 * direction, dest_dev, dest_elem].set(own_global * 6 + 2 * direction + 1)
    return link_table.reshape(6, devices * ELEM_DEV)


def setup_inputs(seed: int = 0) -> dict:
    arg_keys = jax.random.split(jax.random.key(seed), 3)
    solution = draw_solution(jax.random.fold_in(arg_keys[2], 71), 0)
    face_link = draw_face_link(jax.random.fold_in(arg_keys[2], 71), 0)
    return {"solution": solution, "face_link": face_link}


heat_ratio = 1.4
viscosity = 0.08
prandtl = 0.72
penalty = 0.1

def legendre_table(degree, abscissae):
    values = [abscissae * 0.0 + 1.0, abscissae.copy()]
    slopes = [abscissae * 0.0, abscissae * 0.0 + 1.0]
    for current in range(1, degree):
        values.append(((2 * current + 1) * abscissae * values[current] - current * values[current - 1]) / (current + 1))
        slopes.append(slopes[current - 1] + (2 * current + 1) * values[current])
    return (values, slopes)

def gauss_nodes(degree):
    abscissae = np.cos(np.pi * (np.arange(degree) + 0.75) / (degree + 0.5))
    for unused in range(60):
        values, slopes = legendre_table(degree, abscissae)
        abscissae = abscissae - values[degree] / slopes[degree]
    return np.sort(abscissae)

def operator_tables(degree):
    abscissae = gauss_nodes(degree)
    differ = abscissae[:, None] - abscissae[None, :]
    padded = differ + np.eye(degree)
    weights = 1.0 / np.prod(padded, axis=1)
    derivative = weights[None, :] / weights[:, None] / padded * (1.0 - np.eye(degree))
    derivative = derivative - np.eye(degree) * np.sum(derivative, axis=1)[:, None]
    basis_left = weights / (-1.0 - abscissae)
    basis_left = basis_left / np.sum(basis_left)
    basis_right = weights / (1.0 - abscissae)
    basis_right = basis_right / np.sum(basis_right)
    values, slopes = legendre_table(degree, abscissae)
    right_slope = 0.5 * (slopes[degree - 1] + slopes[degree])
    mirror_values, mirror_slopes = legendre_table(degree, -abscissae)
    left_slope = -0.5 * (mirror_slopes[degree - 1] + mirror_slopes[degree])
    sol_points = degree ** 3
    face_points = degree ** 2
    interp = np.zeros((6 * face_points, sol_points))
    grad_matrix = np.zeros((3 * sol_points, sol_points))
    lift_matrix = np.zeros((3 * sol_points, 6 * face_points))
    div_lift = np.zeros((sol_points, 6 * face_points))
    for sol_index in range(sol_points):
        position = (sol_index // face_points, sol_index // degree % degree, sol_index % degree)
        for direction in range(3):
            others = [position[other_dir] for other_dir in range(3) if other_dir != direction]
            flux_index = others[0] * degree + others[1]
            along_index = position[direction]
            for facing in range(2):
                column = (2 * direction + facing) * face_points + flux_index
                interp[column, sol_index] = (basis_left, basis_right)[facing][along_index]
                correct = (left_slope, right_slope)[facing][along_index]
                lift_matrix[direction * sol_points + sol_index, column] = correct
                div_lift[sol_index, column] = (2 * facing - 1) * correct
            for target in range(degree):
                shifted = list(position)
                shifted[direction] = target
                other_point = (shifted[0] * degree + shifted[1]) * degree + shifted[2]
                grad_matrix[direction * sol_points + sol_index, other_point] = derivative[along_index, target]
    normal_matrix = np.zeros((6 * face_points, 3 * sol_points))
    normals = np.zeros((3, 6))
    for face_id in range(6):
        direction = face_id // 2
        orient = 2 * (face_id % 2) - 1
        rows_here = slice(face_id * face_points, (face_id + 1) * face_points)
        normal_matrix[rows_here, direction * sol_points:(direction + 1) * sol_points] = orient * interp[rows_here]
        normals[direction, face_id] = orient
    div_matrix = np.concatenate([grad_matrix[direction * sol_points:(direction + 1) * sol_points] for direction in range(3)], axis=1)
    tables = (interp, grad_matrix, lift_matrix, normal_matrix, div_matrix, div_lift, normals)
    return tuple((jnp.asarray(source, dtype=jnp.float32) for source in tables))

def exact_dot(matrix, operand):
    return jnp.dot(matrix, operand, precision=lax.Precision.HIGHEST, preferred_element_type=jnp.float32)

def face_layout(matrix, face_points, fields, elements):
    return jnp.transpose(matrix.reshape(6, face_points, fields, elements), (1, 2, 0, 3))

def matrix_layout(faces):
    face_points, fields, sides, elements = faces.shape
    return jnp.transpose(faces, (2, 0, 1, 3)).reshape(sides * face_points, fields * elements)

def split_fields(values):
    return [values[:, field_id] for field_id in range(values.shape[1])]

def primitive(fields):
    density = fields[0]
    velocity = [fields[1 + direction] / density for direction in range(3)]
    kinetic = 0.5 * (fields[1] * velocity[0] + fields[2] * velocity[1] + fields[3] * velocity[2])
    pressure = (heat_ratio - 1.0) * (fields[4] - kinetic)
    return (density, velocity, pressure)

def inviscid_flux(fields, velocity, pressure, direction):
    result = [fields[1 + direction]]
    for component in range(3):
        member = fields[1 + component] * velocity[direction]
        if component == direction:
            member = member + pressure
        result.append(member)
    result.append((fields[4] + pressure) * velocity[direction])
    return result

def viscous_terms(fields, density, velocity, slopes):
    vel_slope = [[(slopes[across][1 + component] - velocity[component] * slopes[across][0]) / density for across in range(3)] for component in range(3)]
    energy_slope = []
    for across in range(3):
        internal = (slopes[across][4] - fields[4] / density * slopes[across][0]) / density
        internal = internal - (velocity[0] * vel_slope[0][across] + velocity[1] * vel_slope[1][across] + velocity[2] * vel_slope[2][across])
        energy_slope.append(internal)
    divergence = vel_slope[0][0] + vel_slope[1][1] + vel_slope[2][2]
    return (vel_slope, energy_slope, divergence)

def viscous_flux(velocity, vel_slope, energy_slope, divergence, direction):
    stress = []
    for component in range(3):
        member = viscosity * (vel_slope[component][direction] + vel_slope[direction][component])
        if component == direction:
            member = member - 2.0 / 3.0 * viscosity * divergence
        stress.append(member)
    work_done = velocity[0] * stress[0] + velocity[1] * stress[1] + velocity[2] * stress[2]
    heat_flux = viscosity * heat_ratio / prandtl * energy_slope[direction]
    return [jnp.zeros_like(divergence)] + stress + [work_done + heat_flux]

def total_flux(fields, slopes):
    density, velocity, pressure = primitive(fields)
    vel_slope, energy_slope, divergence = viscous_terms(fields, density, velocity, slopes)
    result = []
    for direction in range(3):
        inviscid = inviscid_flux(fields, velocity, pressure, direction)
        viscous = viscous_flux(velocity, vel_slope, energy_slope, divergence, direction)
        result.append([inviscid[field_id] - viscous[field_id] for field_id in range(5)])
    return result

def normal_viscous(fields, slopes, weights):
    density, velocity, pressure = primitive(fields)
    vel_slope, energy_slope, divergence = viscous_terms(fields, density, velocity, slopes)
    summed = [0.0] * 5
    for direction in range(3):
        viscous = viscous_flux(velocity, vel_slope, energy_slope, divergence, direction)
        summed = [summed[field_id] + weights[direction] * viscous[field_id] for field_id in range(5)]
    return summed

def common_flux(own_fields, other_fields, own_visc, other_visc, weights):
    rho_left, vel_left, press_left = primitive(own_fields)
    rho_right, vel_right, press_right = primitive(other_fields)
    normal_left = [0.0] * 5
    normal_right = [0.0] * 5
    speed_left = 0.0
    speed_right = 0.0
    for direction in range(3):
        flux_left = inviscid_flux(own_fields, vel_left, press_left, direction)
        flux_right = inviscid_flux(other_fields, vel_right, press_right, direction)
        normal_left = [normal_left[field_id] + weights[direction] * flux_left[field_id] for field_id in range(5)]
        normal_right = [normal_right[field_id] + weights[direction] * flux_right[field_id] for field_id in range(5)]
        speed_left = speed_left + weights[direction] * vel_left[direction]
        speed_right = speed_right + weights[direction] * vel_right[direction]
    wave_left = jnp.abs(speed_left) + jnp.sqrt(heat_ratio * press_left / rho_left)
    wave_right = jnp.abs(speed_right) + jnp.sqrt(heat_ratio * press_right / rho_right)
    wave_speed = jnp.maximum(wave_left, wave_right)
    return [0.5 * (normal_left[field_id] + normal_right[field_id]) - 0.5 * (own_visc[field_id] + other_visc[field_id]) + (0.5 * wave_speed + penalty) * (own_fields[field_id] - other_fields[field_id]) for field_id in range(5)]

def reference(solution, face_link):
    interp, grad_matrix, lift_matrix, normal_matrix, div_matrix, div_lift, normals = operator_tables(ORDER + 1)
    sol_points, fields, all_elems = solution.shape
    face_points = (ORDER + 1) ** 2
    elements = ELEM_DEV
    blocks = all_elems // elements
    weights = [normals[direction].reshape(1, 6, 1) for direction in range(3)]
    block_ids = jnp.arange(blocks, dtype=jnp.int32)

    def block_of(values, block_id):
        return lax.dynamic_slice_in_dim(values, block_id * elements, elements, axis=values.ndim - 1)

    def traces(block_id):
        flat_sol = block_of(solution, block_id).reshape(sol_points, fields * elements)
        return face_layout(exact_dot(interp, flat_sol), face_points, fields, elements)
    own_all = lax.map(traces, block_ids)

    def partner(source, block_id):
        link_block = block_of(face_link, block_id)
        partner_elem = link_block // 6
        picked = source[partner_elem // elements, :, :, link_block % 6, partner_elem % elements]
        return jnp.transpose(picked, (2, 3, 0, 1))

    def gradient(block_id):
        flat_sol = block_of(solution, block_id).reshape(sol_points, fields * elements)
        own_trace = own_all[block_id]
        other_trace = partner(own_all, block_id)
        jump_mat = matrix_layout(0.5 * (other_trace - own_trace))
        grad_field = (exact_dot(grad_matrix, flat_sol) + exact_dot(lift_matrix, jump_mat)).reshape(3, sol_points, fields, elements)
        return (own_trace, other_trace, grad_field)

    def viscous_traces(block_id):
        own_trace, other_trace, grad_field = gradient(block_id)
        spread = jnp.einsum('pq,dqx->dpx', interp, grad_field.reshape(3, sol_points, fields * elements), precision=lax.Precision.HIGHEST)
        traced = jnp.transpose(spread.reshape(3, 6, face_points, fields, elements), (0, 2, 3, 1, 4))
        slopes = [split_fields(traced[direction]) for direction in range(3)]
        return jnp.stack(normal_viscous(split_fields(own_trace), slopes, weights), axis=1)
    visc_all = lax.map(viscous_traces, block_ids)

    def rate_block(block_id):
        own_trace, other_trace, grad_field = gradient(block_id)
        own_visc = split_fields(visc_all[block_id])
        other_visc = [-member for member in split_fields(partner(visc_all, block_id))]
        sol_fields = split_fields(block_of(solution, block_id))
        sol_slopes = [split_fields(grad_field[direction]) for direction in range(3)]
        fluxes = total_flux(sol_fields, sol_slopes)
        flux_mat = jnp.stack([jnp.stack(fluxes[direction], axis=1) for direction in range(3)]).reshape(3 * sol_points, fields * elements)
        own_normal = face_layout(exact_dot(normal_matrix, flux_mat), face_points, fields, elements)
        common = common_flux(split_fields(own_trace), split_fields(other_trace), own_visc, other_visc, weights)
        jump_mat = matrix_layout(jnp.stack(common, axis=1) - own_normal)
        return -(exact_dot(div_matrix, flux_mat) + exact_dot(div_lift, jump_mat)).reshape(sol_points, fields, elements)
    block_rates = lax.map(rate_block, block_ids)
    return jnp.transpose(block_rates, (1, 2, 0, 3)).reshape(sol_points, fields, all_elems)
```

```python
import jax
import jax.numpy as jnp
import numpy as np
import functools

from jax import lax
from jax.experimental import pallas as pl
from jax.experimental.pallas import tpu as pltpu
from jax.sharding import PartitionSpec as P

ORDER = 4


heat_ratio = 1.4
viscosity = 0.08
prandtl = 0.72
penalty = 0.1


def legendre_table(degree, abscissae):
    values = [abscissae * 0.0 + 1.0, abscissae.copy()]
    slopes = [abscissae * 0.0, abscissae * 0.0 + 1.0]
    for current in range(1, degree):
        values.append(
            ((2 * current + 1) * abscissae * values[current] - current * values[current - 1])
            / (current + 1)
        )
        slopes.append(slopes[current - 1] + (2 * current + 1) * values[current])
    return (values, slopes)


def gauss_nodes(degree):
    abscissae = np.cos(np.pi * (np.arange(degree) + 0.75) / (degree + 0.5))
    for unused in range(60):
        values, slopes = legendre_table(degree, abscissae)
        abscissae = abscissae - values[degree] / slopes[degree]
    return np.sort(abscissae)


def operator_tables(degree):
    abscissae = gauss_nodes(degree)
    differ = abscissae[:, None] - abscissae[None, :]
    padded = differ + np.eye(degree)
    weights = 1.0 / np.prod(padded, axis=1)
    derivative = weights[None, :] / weights[:, None] / padded * (1.0 - np.eye(degree))
    derivative = derivative - np.eye(degree) * np.sum(derivative, axis=1)[:, None]
    basis_left = weights / (-1.0 - abscissae)
    basis_left = basis_left / np.sum(basis_left)
    basis_right = weights / (1.0 - abscissae)
    basis_right = basis_right / np.sum(basis_right)
    values, slopes = legendre_table(degree, abscissae)
    right_slope = 0.5 * (slopes[degree - 1] + slopes[degree])
    mirror_values, mirror_slopes = legendre_table(degree, -abscissae)
    left_slope = -0.5 * (mirror_slopes[degree - 1] + mirror_slopes[degree])
    sol_points = degree**3
    face_points = degree**2
    interp = np.zeros((6 * face_points, sol_points))
    grad_matrix = np.zeros((3 * sol_points, sol_points))
    lift_matrix = np.zeros((3 * sol_points, 6 * face_points))
    div_lift = np.zeros((sol_points, 6 * face_points))
    for sol_index in range(sol_points):
        position = (sol_index // face_points, sol_index // degree % degree, sol_index % degree)
        for direction in range(3):
            others = [position[other_dir] for other_dir in range(3) if other_dir != direction]
            flux_index = others[0] * degree + others[1]
            along_index = position[direction]
            for facing in range(2):
                column = (2 * direction + facing) * face_points + flux_index
                interp[column, sol_index] = (basis_left, basis_right)[facing][along_index]
                correct = (left_slope, right_slope)[facing][along_index]
                lift_matrix[direction * sol_points + sol_index, column] = correct
                div_lift[sol_index, column] = (2 * facing - 1) * correct
            for target in range(degree):
                shifted = list(position)
                shifted[direction] = target
                other_point = (shifted[0] * degree + shifted[1]) * degree + shifted[2]
                grad_matrix[direction * sol_points + sol_index, other_point] = derivative[
                    along_index, target
                ]
    normal_matrix = np.zeros((6 * face_points, 3 * sol_points))
    normals = np.zeros((3, 6))
    for face_id in range(6):
        direction = face_id // 2
        orient = 2 * (face_id % 2) - 1
        rows_here = slice(face_id * face_points, (face_id + 1) * face_points)
        normal_matrix[rows_here, direction * sol_points : (direction + 1) * sol_points] = (
            orient * interp[rows_here]
        )
        normals[direction, face_id] = orient
    div_matrix = np.concatenate(
        [
            grad_matrix[direction * sol_points : (direction + 1) * sol_points]
            for direction in range(3)
        ],
        axis=1,
    )
    tables = (interp, grad_matrix, lift_matrix, normal_matrix, div_matrix, div_lift, normals)
    return tables


FACE_LANES = 32
LANES = 256
ROWS = 8
MESH = pl.DeviceIdType.MESH


def halves(table):
    high = np.asarray(table, dtype=jnp.bfloat16)
    low = np.asarray(table - high.astype(np.float64), dtype=jnp.bfloat16)
    return (high, low)


def kernel_tables():
    interp, grad_matrix, lift_matrix, normal_matrix, div_matrix, div_lift, normals = (
        operator_tables(ORDER + 1)
    )
    side = ORDER + 1
    points, face_points = side**3, side**2
    width = 128
    to_lanes = np.zeros((6 * face_points, LANES))
    for face_id in range(6):
        for point in range(face_points):
            to_lanes[face_id * face_points + point, face_id * FACE_LANES + point] = 1.0
    filled = to_lanes.copy()
    spare = to_lanes.sum(axis=0) == 0.0
    filled[0, spare] = 1.0
    trace = np.zeros((width, LANES))
    trace[:points] = interp.T @ filled
    own_grad = np.zeros((width, 3 * width))
    own_spread = np.zeros((width, 3 * LANES))
    jump_grad = np.zeros((LANES, 3 * width))
    jump_spread = np.zeros((LANES, 3 * LANES))
    div = np.zeros((3 * width, width))
    div_all = div_matrix - div_lift @ normal_matrix
    for direction in range(3):
        rows = slice(direction * points, (direction + 1) * points)
        cols = slice(direction * width, direction * width + points)
        wide = slice(direction * LANES, (direction + 1) * LANES)
        own_grad[:points, cols] = grad_matrix[rows].T
        own_spread[:points, wide] = (interp @ grad_matrix[rows]).T @ to_lanes
        jump_grad[:, cols] = to_lanes.T @ (0.5 * lift_matrix[rows]).T
        jump_spread[:, wide] = to_lanes.T @ (interp @ (0.5 * lift_matrix[rows])).T @ to_lanes
        div[cols, :points] = div_all[:, rows].T
    lift = np.zeros((LANES, width))
    lift[:, :points] = to_lanes.T @ div_lift.T
    result = []
    for table in (trace, own_grad, own_spread, jump_grad, jump_spread, div, lift):
        result.extend(halves(table))
    weights = np.zeros((8, LANES), np.float32)
    for direction in range(3):
        for face_id in range(6):
            start = face_id * FACE_LANES
            weights[direction, start : start + FACE_LANES] = normals[direction, face_id]
    return result + [weights]


def split(value):
    high = value.astype(jnp.bfloat16)
    low = (value - high.astype(jnp.float32)).astype(jnp.bfloat16)
    return (high, low)


def mxu(left, right):
    return jnp.dot(left, right, preferred_element_type=jnp.float32)


def table_dot(parts, high, low):
    return mxu(parts[0], high) + mxu(parts[1], high) + mxu(parts[0], low)


def pick_dot(picks, parts):
    return mxu(picks, parts[0]) + mxu(picks, parts[1])


def faces_first(blocks, lane, elements):
    per_face = []
    for face_id in range(6):
        tile, inner = divmod(face_id * FACE_LANES, 128)
        total = jnp.zeros((elements, 128), jnp.float32)
        for field_id, block in enumerate(blocks):
            if block is None:
                continue
            shift = (25 * field_id - inner) % 128
            piece = block[:, tile * 128 : tile * 128 + 128]
            if shift:
                piece = pltpu.roll(piece, shift, 1)
            mine = (lane >= 25 * field_id) & (lane < 25 * field_id + 25)
            total = jnp.where(mine, piece, total)
        per_face.append(total)
    return jnp.concatenate(per_face, axis=0)


def fields_first(rows, lane, elements, field_ids, base):
    result = []
    for field_id in field_ids:
        tiles = []
        for tile in range(2):
            total = base[field_id][:, tile * 128 : tile * 128 + 128]
            for face_id in range(tile * 4, min(6, tile * 4 + 4)):
                inner = face_id * FACE_LANES - tile * 128
                shift = (inner - 25 * field_id) % 128
                piece = rows[face_id * elements : (face_id + 1) * elements]
                if shift:
                    piece = pltpu.roll(piece, shift, 1)
                mine = (lane >= inner) & (lane < inner + 25)
                total = jnp.where(mine, piece, total)
            tiles.append(total)
        result.append(jnp.concatenate(tiles, axis=1))
    return result


def divided(value, count):
    return jnp.floor((value + 0.5) * (1.0 / count))


def state_of(fields):
    inverse = 1.0 / fields[0]
    velocity = [fields[1 + b] * inverse for b in range(3)]
    kinetic = 0.5 * (fields[1] * velocity[0] + fields[2] * velocity[1] + fields[3] * velocity[2])
    pressure = (heat_ratio - 1.0) * (fields[4] - kinetic)
    return (inverse, velocity, pressure)


def normal_inviscid(fields, velocity, pressure, normal):
    speed = sum(normal[b] * velocity[b] for b in range(3))
    momentum = sum(normal[b] * fields[1 + b] for b in range(3))
    flux = [momentum]
    for b in range(3):
        flux.append(fields[1 + b] * speed + pressure * normal[b])
    flux.append((fields[4] + pressure) * speed)
    return (flux, speed)


def slopes_of(fields, inverse, velocity, grads):
    slope = [
        [(grads[a][1 + b] - velocity[b] * grads[a][0]) * inverse for a in range(3)]
        for b in range(3)
    ]
    specific = fields[4] * inverse
    energy = []
    for a in range(3):
        value = (grads[a][4] - specific * grads[a][0]) * inverse
        energy.append(value - sum(velocity[b] * slope[b][a] for b in range(3)))
    return (slope, energy)


def body(shape, *refs):
    elements, capacity, sub_count, dom_count = shape
    sol_ref, link_ref = refs[:2]
    (trace_h, trace_l, own_grad_h, own_grad_l, own_spread_h, own_spread_l, jump_grad_h,
     jump_grad_l, jump_spread_h, jump_spread_l, div_h, div_l, lift_h, lift_l) = refs[2:16]
    weights_ref, out_ref, padded, outbox, inbox, send_sem, recv_sem = refs[16:]
    my_dom, my_sub = lax.axis_index("dom"), lax.axis_index("sub")
    home = 2 * sub_count
    groups = 5 * sub_count
    partners = []
    for offset in range(-2, 3):
        for across in range(sub_count):
            if offset == 0 and across == 0:
                continue
            there = (
                lax.rem(my_dom + offset + dom_count, dom_count),
                lax.rem(my_sub + across, sub_count),
            )
            group = (offset + 2) * sub_count + across
            mirror = (2 - offset) * sub_count + (-across) % sub_count
            partners.append((group, mirror, there))
    barrier = pltpu.get_barrier_semaphore()
    for _, _, there in partners:
        pl.semaphore_signal(barrier, inc=1, device_id=there, device_id_type=MESH)

    def ship(turn):
        copies = []
        for group, mirror, there in partners:
            copies.append(
                pltpu.make_async_remote_copy(
                    src_ref=outbox.at[turn, group],
                    dst_ref=inbox.at[turn, mirror],
                    send_sem=send_sem.at[turn, group],
                    recv_sem=recv_sem.at[turn, mirror],
                    device_id=there,
                    device_id_type=MESH,
                )
            )
            copies[-1].start()
        return copies

    faces = 6 * elements
    slots = groups * ROWS
    points = sol_ref.shape[2]
    lane = lax.broadcasted_iota(jnp.int32, (elements, 128), 1)

    for k in range(5):
        here = sol_ref[k]
        padded[k * elements : (k + 1) * elements, :points] = here
        padded[k * elements : (k + 1) * elements, points:] = here[:, : 128 - points]
    state = padded[...]
    state_parts = split(state)
    own = table_dot(state_parts, trace_h[...], trace_l[...])

    def by_field(values, start=0, width=LANES):
        return [
            values[k * elements : (k + 1) * elements, start : start + width] for k in range(5)
        ]

    own_fields = by_field(own)
    own_rows = faces_first(own_fields, lane, elements)
    own_parts = split(own_rows)

    link = link_ref[...].astype(jnp.float32)
    elem = divided(link, 6)
    side = link - 6.0 * elem
    device = divided(elem, elements)
    key = side * elements + (elem - device * elements)
    dom = divided(device, sub_count)
    sub = device - dom * sub_count
    ahead = dom - my_dom.astype(jnp.float32) + 2.0
    ahead = jnp.where(ahead < 0.0, ahead + dom_count, ahead)
    ahead = jnp.where(ahead >= dom_count, ahead - dom_count, ahead)
    across = sub - my_sub.astype(jnp.float32)
    across = jnp.where(across < 0.0, across + sub_count, across)
    group = ahead * sub_count + across

    def as_row(value):
        return jnp.concatenate([value[f : f + 1] for f in range(6)], axis=1)

    group_row = as_row(group)
    key_row = as_row(key)
    both = jnp.concatenate([group_row, key_row] + [group_row] * 6, axis=0).T
    group_col = both[:, 0:1]
    key_col = both[:, 1:2]
    down = lax.broadcasted_iota(jnp.int32, (faces, faces), 0)
    along = lax.broadcasted_iota(jnp.int32, (faces, faces), 1)
    same = group_col == group_row
    send_rank = jnp.sum(jnp.where(same & (down < along), 1.0, 0.0), axis=0, keepdims=True)
    send_slot = jnp.where(group_row == home, -1.0, group_row * ROWS + send_rank)
    slot_down = lax.broadcasted_iota(jnp.int32, (slots, faces), 0).astype(jnp.float32)
    send_pick = jnp.where(send_slot == slot_down, 1.0, 0.0).astype(jnp.bfloat16)

    outbox[0] = pick_dot(send_pick, own_parts).reshape(groups, ROWS, 128)
    pl.semaphore_wait(barrier, len(partners))
    first = ship(0)

    recv_rank = jnp.sum(jnp.where(same & (key_row < key_col), 1.0, 0.0), axis=1, keepdims=True)
    recv_slot = jnp.where(group_col == home, -1.0, group_col * ROWS + recv_rank)
    slot_along = lax.broadcasted_iota(jnp.int32, (faces, slots), 1).astype(jnp.float32)
    recv_pick = jnp.where(recv_slot == slot_along, 1.0, 0.0).astype(jnp.bfloat16)
    near_key = jnp.where(group_col == home, key_col, -1.0)
    near_pick = jnp.where(near_key == along.astype(jnp.float32), 1.0, 0.0).astype(jnp.bfloat16)

    near_rows = pick_dot(near_pick, own_parts)
    own_spread = table_dot(state_parts, own_spread_h[...], own_spread_l[...])
    own_grad = table_dot(state_parts, own_grad_h[...], own_grad_l[...])
    normal = [weights_ref[a : a + 1] for a in range(3)]
    inverse, velocity, pressure = state_of(own_fields)
    own_flux, own_speed = normal_inviscid(own_fields, velocity, pressure, normal)
    own_wave = jnp.abs(own_speed) + jnp.sqrt(heat_ratio * pressure * inverse)

    inbox[0, home] = jnp.zeros((ROWS, 128), jnp.float32)
    inbox[1, home] = jnp.zeros((ROWS, 128), jnp.float32)
    for copy in first:
        copy.wait_recv()
    arrived = split(inbox[0].reshape(slots, 128))
    other_rows = near_rows + pick_dot(recv_pick, arrived)
    other_fields = fields_first(other_rows, lane, elements, range(5), own_fields)
    jump = jnp.concatenate([other_fields[k] - own_fields[k] for k in range(5)], axis=0)
    jump_parts = split(jump)
    spread = own_spread + table_dot(jump_parts, jump_spread_h[...], jump_spread_l[...])
    grads = [by_field(spread, a * LANES) for a in range(3)]

    slope, energy = slopes_of(own_fields, inverse, velocity, grads)
    divergence = slope[0][0] + slope[1][1] + slope[2][2]
    own_visc = [None]
    for b in range(3):
        stress = sum(normal[a] * (slope[b][a] + slope[a][b]) for a in range(3))
        own_visc.append(viscosity * stress - (2.0 / 3.0 * viscosity) * normal[b] * divergence)
    heat = sum(normal[a] * energy[a] for a in range(3))
    own_visc.append(
        sum(velocity[b] * own_visc[1 + b] for b in range(3))
        + (viscosity * heat_ratio / prandtl) * heat
    )
    visc_rows = faces_first(own_visc, lane, elements)
    visc_parts = split(visc_rows)
    outbox[1] = pick_dot(send_pick, visc_parts).reshape(groups, ROWS, 128)
    second = ship(1)

    near_visc = pick_dot(near_pick, visc_parts)
    grad = own_grad + table_dot(jump_parts, jump_grad_h[...], jump_grad_l[...])
    grads = [by_field(grad, a * 128, 128) for a in range(3)]
    fields = by_field(state, 0, 128)
    inner_inverse, inner_velocity, inner_pressure = state_of(fields)
    slope, energy = slopes_of(fields, inner_inverse, inner_velocity, grads)
    divergence = (2.0 / 3.0 * viscosity) * (slope[0][0] + slope[1][1] + slope[2][2])
    total = None
    for a in range(3):
        stress = []
        for b in range(3):
            if a == b:
                stress.append((2.0 * viscosity) * slope[a][a] - divergence)
            else:
                stress.append(viscosity * (slope[b][a] + slope[a][b]))
        flux = [fields[1 + a]]
        for b in range(3):
            member = fields[1 + b] * inner_velocity[a] - stress[b]
            flux.append(member + inner_pressure if a == b else member)
        flux.append(
            (fields[4] + inner_pressure) * inner_velocity[a]
            - sum(inner_velocity[b] * stress[b] for b in range(3))
            - (viscosity * heat_ratio / prandtl) * energy[a]
        )
        flux_parts = split(jnp.concatenate(flux, axis=0))
        rows = slice(a * 128, (a + 1) * 128)
        part = table_dot(flux_parts, div_h[rows], div_l[rows])
        total = part if total is None else total + part

    other_inverse, other_velocity, other_pressure = state_of(other_fields)
    other_flux, other_speed = normal_inviscid(
        other_fields, other_velocity, other_pressure, normal
    )
    other_wave = jnp.abs(other_speed) + jnp.sqrt(heat_ratio * other_pressure * other_inverse)
    factor = 0.5 * jnp.maximum(own_wave, other_wave) + penalty
    common = []
    for k in range(5):
        member = 0.5 * (own_flux[k] + other_flux[k]) + factor * (own_fields[k] - other_fields[k])
        common.append(member if k == 0 else member - 0.5 * own_visc[k])
    total = total + table_dot(split(jnp.concatenate(common, axis=0)), lift_h[...], lift_l[...])

    for copy in second:
        copy.wait_recv()
    arrived = split(0.5 * inbox[1].reshape(slots, 128))
    other_rows = 0.5 * near_visc + pick_dot(recv_pick, arrived)
    zeros = [jnp.zeros((elements, LANES), jnp.float32)] * 5
    other_visc = fields_first(other_rows, lane, elements, range(1, 5), zeros)
    lifted = table_dot(split(jnp.concatenate(other_visc, axis=0)), lift_h[...], lift_l[...])
    out_ref[0] = -total[:elements, :points]
    for k in range(1, 5):
        rows = slice(k * elements, (k + 1) * elements)
        near = slice((k - 1) * elements, k * elements)
        out_ref[k] = -(total[rows, :points] + lifted[near, :points])
    for copy in first + second:
        copy.wait_send()


def shards(solution, face_link):
    points, fields, elements = solution.shape
    sub_count = lax.axis_size("sub")
    dom_count = lax.axis_size("dom")
    capacity = max(3, elements * 3 // 16)
    assert capacity <= ROWS
    groups = 5 * sub_count
    tables = [jnp.asarray(table) for table in kernel_tables()]
    vmem = pl.BlockSpec(memory_space=pltpu.VMEM)
    rate = pl.pallas_call(
        functools.partial(body, (elements, capacity, sub_count, dom_count)),
        out_shape=jax.ShapeDtypeStruct((fields, elements, points), jnp.float32),
        in_specs=[vmem] * (2 + len(tables)),
        out_specs=vmem,
        scratch_shapes=[
            pltpu.VMEM((fields * elements, 128), jnp.float32),
            pltpu.VMEM((2, groups, ROWS, 128), jnp.float32),
            pltpu.VMEM((2, groups, ROWS, 128), jnp.float32),
            pltpu.SemaphoreType.DMA((2, groups)),
            pltpu.SemaphoreType.DMA((2, groups)),
        ],
        compiler_params=pltpu.CompilerParams(collective_id=0, has_side_effects=True),
    )(jnp.transpose(solution, (1, 2, 0)), face_link, *tables)
    return jnp.transpose(rate, (2, 0, 1))


def solution(mesh):
    in_specs = (P(None, None, ("dom", "sub")), P(None, ("dom", "sub")))
    out_specs = P(None, None, ("dom", "sub"))
    return jax.shard_map(shards, mesh=mesh, in_specs=in_specs, out_specs=out_specs, check_vma=False)
```

```python
import jax
import jax.numpy as jnp
import numpy as np
import functools

from jax import lax
from jax.experimental import pallas as pl
from jax.experimental.pallas import tpu as pltpu
from jax.sharding import PartitionSpec as P

ORDER = 4


heat_ratio = 1.4
viscosity = 0.08
prandtl = 0.72
penalty = 0.1


def legendre_table(degree, abscissae):
    values = [abscissae * 0.0 + 1.0, abscissae.copy()]
    slopes = [abscissae * 0.0, abscissae * 0.0 + 1.0]
    for current in range(1, degree):
        values.append(
            ((2 * current + 1) * abscissae * values[current] - current * values[current - 1])
            / (current + 1)
        )
        slopes.append(slopes[current - 1] + (2 * current + 1) * values[current])
    return (values, slopes)


def gauss_nodes(degree):
    abscissae = np.cos(np.pi * (np.arange(degree) + 0.75) / (degree + 0.5))
    for unused in range(60):
        values, slopes = legendre_table(degree, abscissae)
        abscissae = abscissae - values[degree] / slopes[degree]
    return np.sort(abscissae)


def operator_tables(degree):
    abscissae = gauss_nodes(degree)
    differ = abscissae[:, None] - abscissae[None, :]
    padded = differ + np.eye(degree)
    weights = 1.0 / np.prod(padded, axis=1)
    derivative = weights[None, :] / weights[:, None] / padded * (1.0 - np.eye(degree))
    derivative = derivative - np.eye(degree) * np.sum(derivative, axis=1)[:, None]
    basis_left = weights / (-1.0 - abscissae)
    basis_left = basis_left / np.sum(basis_left)
    basis_right = weights / (1.0 - abscissae)
    basis_right = basis_right / np.sum(basis_right)
    values, slopes = legendre_table(degree, abscissae)
    right_slope = 0.5 * (slopes[degree - 1] + slopes[degree])
    mirror_values, mirror_slopes = legendre_table(degree, -abscissae)
    left_slope = -0.5 * (mirror_slopes[degree - 1] + mirror_slopes[degree])
    sol_points = degree**3
    face_points = degree**2
    interp = np.zeros((6 * face_points, sol_points))
    grad_matrix = np.zeros((3 * sol_points, sol_points))
    lift_matrix = np.zeros((3 * sol_points, 6 * face_points))
    div_lift = np.zeros((sol_points, 6 * face_points))
    for sol_index in range(sol_points):
        position = (sol_index // face_points, sol_index // degree % degree, sol_index % degree)
        for direction in range(3):
            others = [position[other_dir] for other_dir in range(3) if other_dir != direction]
            flux_index = others[0] * degree + others[1]
            along_index = position[direction]
            for facing in range(2):
                column = (2 * direction + facing) * face_points + flux_index
                interp[column, sol_index] = (basis_left, basis_right)[facing][along_index]
                correct = (left_slope, right_slope)[facing][along_index]
                lift_matrix[direction * sol_points + sol_index, column] = correct
                div_lift[sol_index, column] = (2 * facing - 1) * correct
            for target in range(degree):
                shifted = list(position)
                shifted[direction] = target
                other_point = (shifted[0] * degree + shifted[1]) * degree + shifted[2]
                grad_matrix[direction * sol_points + sol_index, other_point] = derivative[
                    along_index, target
                ]
    normal_matrix = np.zeros((6 * face_points, 3 * sol_points))
    normals = np.zeros((3, 6))
    for face_id in range(6):
        direction = face_id // 2
        orient = 2 * (face_id % 2) - 1
        rows_here = slice(face_id * face_points, (face_id + 1) * face_points)
        normal_matrix[rows_here, direction * sol_points : (direction + 1) * sol_points] = (
            orient * interp[rows_here]
        )
        normals[direction, face_id] = orient
    div_matrix = np.concatenate(
        [
            grad_matrix[direction * sol_points : (direction + 1) * sol_points]
            for direction in range(3)
        ],
        axis=1,
    )
    tables = (interp, grad_matrix, lift_matrix, normal_matrix, div_matrix, div_lift, normals)
    return tables


FACE_LANES = 32
LANES = 256
ROWS = 8
MESH = pl.DeviceIdType.MESH


def halves(table):
    high = np.asarray(table, dtype=jnp.bfloat16)
    low = np.asarray(table - high.astype(np.float64), dtype=jnp.bfloat16)
    return (high, low)


def kernel_tables():
    interp, grad_matrix, lift_matrix, normal_matrix, div_matrix, div_lift, normals = (
        operator_tables(ORDER + 1)
    )
    side = ORDER + 1
    points, face_points = side**3, side**2
    width = 128
    to_lanes = np.zeros((6 * face_points, LANES))
    for face_id in range(6):
        for point in range(face_points):
            to_lanes[face_id * face_points + point, face_id * FACE_LANES + point] = 1.0
    filled = to_lanes.copy()
    spare = to_lanes.sum(axis=0) == 0.0
    filled[0, spare] = 1.0
    trace = np.zeros((width, LANES))
    trace[:points] = interp.T @ filled
    own_grad = np.zeros((width, 3 * width))
    own_spread = np.zeros((width, 3 * LANES))
    jump_grad = np.zeros((LANES, 3 * width))
    jump_spread = np.zeros((LANES, 3 * LANES))
    div = np.zeros((3 * width, width))
    div_all = div_matrix - div_lift @ normal_matrix
    for direction in range(3):
        rows = slice(direction * points, (direction + 1) * points)
        cols = slice(direction * width, direction * width + points)
        wide = slice(direction * LANES, (direction + 1) * LANES)
        own_grad[:points, cols] = grad_matrix[rows].T
        own_spread[:points, wide] = (interp @ grad_matrix[rows]).T @ to_lanes
        jump_grad[:, cols] = to_lanes.T @ (0.5 * lift_matrix[rows]).T
        jump_spread[:, wide] = to_lanes.T @ (interp @ (0.5 * lift_matrix[rows])).T @ to_lanes
        div[cols, :points] = div_all[:, rows].T
    lift = np.zeros((LANES, width))
    lift[:, :points] = to_lanes.T @ div_lift.T
    result = []
    for table in (trace, own_grad, own_spread, jump_grad, jump_spread, div, lift):
        result.append(np.stack(halves(table)))
    weights = np.zeros((8, LANES), np.float32)
    for direction in range(3):
        for face_id in range(6):
            start = face_id * FACE_LANES
            weights[direction, start : start + FACE_LANES] = normals[direction, face_id]
    return result + [weights]


def split(value):
    high = value.astype(jnp.bfloat16)
    low = (value - high.astype(jnp.float32)).astype(jnp.bfloat16)
    return (high, low)


def thirds(value):
    high, low = split(value)
    rest = value - high.astype(jnp.float32) - low.astype(jnp.float32)
    return (high, low, rest.astype(jnp.bfloat16))


def mxu(left, right):
    return jnp.dot(left, right, preferred_element_type=jnp.float32)


def table_dot(parts, high, low):
    return mxu(parts[0], high) + mxu(parts[1], high) + mxu(parts[0], low)


def pick_dot(picks, parts):
    return sum(mxu(picks, part) for part in parts)


def faces_first(blocks, lane, elements):
    per_face = []
    for face_id in range(6):
        tile, inner = divmod(face_id * FACE_LANES, 128)
        total = jnp.zeros((elements, 128), jnp.float32)
        for field_id, block in enumerate(blocks):
            if block is None:
                continue
            shift = (25 * field_id - inner) % 128
            piece = block[:, tile * 128 : tile * 128 + 128]
            if shift:
                piece = pltpu.roll(piece, shift, 1)
            mine = (lane >= 25 * field_id) & (lane < 25 * field_id + 25)
            total = jnp.where(mine, piece, total)
        per_face.append(total)
    return jnp.concatenate(per_face, axis=0)


def fields_first(rows, lane, elements, field_ids, base):
    result = []
    for field_id in field_ids:
        tiles = []
        for tile in range(2):
            total = base[field_id][:, tile * 128 : tile * 128 + 128]
            for face_id in range(tile * 4, min(6, tile * 4 + 4)):
                inner = face_id * FACE_LANES - tile * 128
                shift = (inner - 25 * field_id) % 128
                piece = rows[face_id * elements : (face_id + 1) * elements]
                if shift:
                    piece = pltpu.roll(piece, shift, 1)
                mine = (lane >= inner) & (lane < inner + 25)
                total = jnp.where(mine, piece, total)
            tiles.append(total)
        result.append(jnp.concatenate(tiles, axis=1))
    return result


def divided(value, count):
    return jnp.floor((value + 0.5) * (1.0 / count))


def state_of(fields):
    inverse = 1.0 / fields[0]
    velocity = [fields[1 + b] * inverse for b in range(3)]
    kinetic = 0.5 * (fields[1] * velocity[0] + fields[2] * velocity[1] + fields[3] * velocity[2])
    pressure = (heat_ratio - 1.0) * (fields[4] - kinetic)
    return (inverse, velocity, pressure)


def normal_inviscid(fields, velocity, pressure, normal):
    speed = sum(normal[b] * velocity[b] for b in range(3))
    momentum = sum(normal[b] * fields[1 + b] for b in range(3))
    flux = [momentum]
    for b in range(3):
        flux.append(fields[1 + b] * speed + pressure * normal[b])
    flux.append((fields[4] + pressure) * speed)
    return (flux, speed)


def slopes_of(fields, inverse, velocity, grads):
    slope = [
        [(grads[a][1 + b] - velocity[b] * grads[a][0]) * inverse for a in range(3)]
        for b in range(3)
    ]
    specific = fields[4] * inverse
    energy = []
    for a in range(3):
        value = (grads[a][4] - specific * grads[a][0]) * inverse
        energy.append(value - sum(velocity[b] * slope[b][a] for b in range(3)))
    return (slope, energy)


def body(shape, *refs):
    elements, capacity, sub_count, dom_count = shape
    far, out_ref, held = refs[:10], refs[10], refs[11:21]
    padded, outbox, inbox, load_sem, send_sem, recv_sem = refs[21:]
    sol_ref, link_ref, trace, own_grad_t, own_spread_t, jump_grad, jump_spread, div, lift = held[:9]
    weights_ref = held[9]
    my_dom, my_sub = lax.axis_index("dom"), lax.axis_index("sub")
    home = 2 * sub_count
    groups = 5 * sub_count
    partners = []
    for offset in range(-2, 3):
        for across in range(sub_count):
            if offset == 0 and across == 0:
                continue
            there = (
                lax.rem(my_dom + offset + dom_count, dom_count),
                lax.rem(my_sub + across, sub_count),
            )
            group = (offset + 2) * sub_count + across
            mirror = (2 - offset) * sub_count + (-across) % sub_count
            partners.append((group, mirror, there))
    barrier = pltpu.get_barrier_semaphore()
    for _, _, there in partners:
        pl.semaphore_signal(barrier, inc=1, device_id=there, device_id_type=MESH)

    def ship(turn):
        copies = []
        for group, mirror, there in partners:
            copies.append(
                pltpu.make_async_remote_copy(
                    src_ref=outbox.at[turn, group],
                    dst_ref=inbox.at[turn, mirror],
                    send_sem=send_sem.at[turn, group],
                    recv_sem=recv_sem.at[turn, mirror],
                    device_id=there,
                    device_id_type=MESH,
                )
            )
            copies[-1].start()
        return copies

    loads = [
        pltpu.make_async_copy(far[i], held[i], load_sem.at[i])
        for i in range(10)
    ]
    for i in (0, 1, 2, 4, 3, 9, 6, 5, 7, 8):
        loads[i].start()

    def loaded(*which):
        for i in which:
            loads[i].wait()

    faces = 6 * elements
    slots = groups * ROWS
    points = sol_ref.shape[2]
    lane = lax.broadcasted_iota(jnp.int32, (elements, 128), 1)

    loaded(0, 2)
    for k in range(5):
        here = sol_ref[k]
        padded[k * elements : (k + 1) * elements, :points] = here
        padded[k * elements : (k + 1) * elements, points:] = here[:, : 128 - points]
    state = padded[...]
    state_parts = split(state)
    own = table_dot(state_parts, trace[0], trace[1])

    def by_field(values, start=0, width=LANES):
        return [
            values[k * elements : (k + 1) * elements, start : start + width] for k in range(5)
        ]

    own_fields = by_field(own)
    own_rows = faces_first(own_fields, lane, elements)
    own_parts = thirds(own_rows)

    loaded(1)
    link = link_ref[...].astype(jnp.float32)
    elem = divided(link, 6)
    side = link - 6.0 * elem
    device = divided(elem, elements)
    key = side * elements + (elem - device * elements)
    dom = divided(device, sub_count)
    sub = device - dom * sub_count
    ahead = dom - my_dom.astype(jnp.float32) + 2.0
    ahead = jnp.where(ahead < 0.0, ahead + dom_count, ahead)
    ahead = jnp.where(ahead >= dom_count, ahead - dom_count, ahead)
    across = sub - my_sub.astype(jnp.float32)
    across = jnp.where(across < 0.0, across + sub_count, across)
    group = ahead * sub_count + across

    def as_row(value):
        return jnp.concatenate([value[f : f + 1] for f in range(6)], axis=1)

    group_row = as_row(group)
    key_row = as_row(key)
    both = jnp.concatenate([group_row, key_row] + [group_row] * 6, axis=0).T
    group_col = both[:, 0:1]
    key_col = both[:, 1:2]
    down = lax.broadcasted_iota(jnp.int32, (faces, faces), 0)
    along = lax.broadcasted_iota(jnp.int32, (faces, faces), 1)
    same = group_col == group_row
    send_rank = jnp.sum(jnp.where(same & (down < along), 1.0, 0.0), axis=0, keepdims=True)
    send_slot = jnp.where(group_row == home, -1.0, group_row * ROWS + send_rank)
    slot_down = lax.broadcasted_iota(jnp.int32, (slots, faces), 0).astype(jnp.float32)
    send_pick = jnp.where(send_slot == slot_down, 1.0, 0.0).astype(jnp.bfloat16)

    outbox[0] = pick_dot(send_pick, own_parts).reshape(groups, ROWS, 128)
    pl.semaphore_wait(barrier, len(partners))
    first = ship(0)

    recv_rank = jnp.sum(jnp.where(same & (key_row < key_col), 1.0, 0.0), axis=1, keepdims=True)
    recv_slot = jnp.where(group_col == home, -1.0, group_col * ROWS + recv_rank)
    slot_along = lax.broadcasted_iota(jnp.int32, (faces, slots), 1).astype(jnp.float32)
    recv_pick = jnp.where(recv_slot == slot_along, 1.0, 0.0).astype(jnp.bfloat16)
    near_key = jnp.where(group_col == home, key_col, -1.0)
    near_pick = jnp.where(near_key == along.astype(jnp.float32), 1.0, 0.0).astype(jnp.bfloat16)

    near_rows = pick_dot(near_pick, own_parts)
    loaded(4, 3, 9)
    own_spread = table_dot(state_parts, own_spread_t[0], own_spread_t[1])
    own_grad = table_dot(state_parts, own_grad_t[0], own_grad_t[1])
    normal = [weights_ref[a : a + 1] for a in range(3)]
    inverse, velocity, pressure = state_of(own_fields)
    own_flux, own_speed = normal_inviscid(own_fields, velocity, pressure, normal)
    own_wave = jnp.abs(own_speed) + jnp.sqrt(heat_ratio * pressure * inverse)

    loaded(6)
    inbox[0, home] = jnp.zeros((ROWS, 128), jnp.float32)
    inbox[1, home] = jnp.zeros((ROWS, 128), jnp.float32)
    for copy in first:
        copy.wait_recv()
    arrived = thirds(inbox[0].reshape(slots, 128))
    other_rows = near_rows + pick_dot(recv_pick, arrived)
    other_fields = fields_first(other_rows, lane, elements, range(5), own_fields)
    jump = jnp.concatenate([other_fields[k] - own_fields[k] for k in range(5)], axis=0)
    jump_parts = split(jump)
    spread = own_spread + table_dot(jump_parts, jump_spread[0], jump_spread[1])
    grads = [by_field(spread, a * LANES) for a in range(3)]

    slope, energy = slopes_of(own_fields, inverse, velocity, grads)
    divergence = slope[0][0] + slope[1][1] + slope[2][2]
    own_visc = [None]
    for b in range(3):
        stress = sum(normal[a] * (slope[b][a] + slope[a][b]) for a in range(3))
        own_visc.append(viscosity * stress - (2.0 / 3.0 * viscosity) * normal[b] * divergence)
    heat = sum(normal[a] * energy[a] for a in range(3))
    own_visc.append(
        sum(velocity[b] * own_visc[1 + b] for b in range(3))
        + (viscosity * heat_ratio / prandtl) * heat
    )
    visc_rows = faces_first(own_visc, lane, elements)
    visc_parts = split(visc_rows)
    outbox[1] = pick_dot(send_pick, visc_parts).reshape(groups, ROWS, 128)
    second = ship(1)

    loaded(5, 7, 8)
    near_visc = pick_dot(near_pick, visc_parts)
    grad = own_grad + table_dot(jump_parts, jump_grad[0], jump_grad[1])
    grads = [by_field(grad, a * 128, 128) for a in range(3)]
    fields = by_field(state, 0, 128)
    inner_inverse, inner_velocity, inner_pressure = state_of(fields)
    slope, energy = slopes_of(fields, inner_inverse, inner_velocity, grads)
    divergence = (2.0 / 3.0 * viscosity) * (slope[0][0] + slope[1][1] + slope[2][2])
    total = None
    for a in range(3):
        stress = []
        for b in range(3):
            if a == b:
                stress.append((2.0 * viscosity) * slope[a][a] - divergence)
            else:
                stress.append(viscosity * (slope[b][a] + slope[a][b]))
        flux = [fields[1 + a]]
        for b in range(3):
            member = fields[1 + b] * inner_velocity[a] - stress[b]
            flux.append(member + inner_pressure if a == b else member)
        flux.append(
            (fields[4] + inner_pressure) * inner_velocity[a]
            - sum(inner_velocity[b] * stress[b] for b in range(3))
            - (viscosity * heat_ratio / prandtl) * energy[a]
        )
        flux_parts = split(jnp.concatenate(flux, axis=0))
        rows = slice(a * 128, (a + 1) * 128)
        part = table_dot(flux_parts, div[0, rows], div[1, rows])
        total = part if total is None else total + part

    other_inverse, other_velocity, other_pressure = state_of(other_fields)
    other_flux, other_speed = normal_inviscid(
        other_fields, other_velocity, other_pressure, normal
    )
    other_wave = jnp.abs(other_speed) + jnp.sqrt(heat_ratio * other_pressure * other_inverse)
    factor = 0.5 * jnp.maximum(own_wave, other_wave) + penalty
    common = []
    for k in range(5):
        member = 0.5 * (own_flux[k] + other_flux[k]) + factor * (own_fields[k] - other_fields[k])
        common.append(member if k == 0 else member - 0.5 * own_visc[k])
    total = total + table_dot(split(jnp.concatenate(common, axis=0)), lift[0], lift[1])

    for copy in second:
        copy.wait_recv()
    arrived = split(0.5 * inbox[1].reshape(slots, 128))
    other_rows = 0.5 * near_visc + pick_dot(recv_pick, arrived)
    zeros = [jnp.zeros((elements, LANES), jnp.float32)] * 5
    other_visc = fields_first(other_rows, lane, elements, range(1, 5), zeros)
    lifted = table_dot(split(jnp.concatenate(other_visc, axis=0)), lift[0], lift[1])
    out_ref[0] = total[:elements, :points]
    for k in range(1, 5):
        rows = slice(k * elements, (k + 1) * elements)
        near = slice((k - 1) * elements, k * elements)
        out_ref[k] = total[rows, :points] + lifted[near, :points]
    for copy in first + second:
        copy.wait_send()


def shards(solution, face_link):
    points, fields, elements = solution.shape
    sub_count = lax.axis_size("sub")
    dom_count = lax.axis_size("dom")
    capacity = max(3, elements * 3 // 16)
    assert capacity <= ROWS
    groups = 5 * sub_count
    tables = [jnp.asarray(table) for table in kernel_tables()]
    vmem = pl.BlockSpec(memory_space=pltpu.VMEM)
    operands = [jnp.transpose(solution, (1, 2, 0)), face_link] + tables
    held = [pltpu.VMEM(operand.shape, operand.dtype) for operand in operands]
    rate = pl.pallas_call(
        functools.partial(body, (elements, capacity, sub_count, dom_count)),
        out_shape=pltpu.VMEM((fields, elements, points), jnp.float32),
        in_specs=[pl.BlockSpec(memory_space=pltpu.HBM)] * len(operands),
        out_specs=vmem,
        scratch_shapes=held + [
            pltpu.VMEM((fields * elements, 128), jnp.float32),
            pltpu.VMEM((2, groups, ROWS, 128), jnp.float32),
            pltpu.VMEM((2, groups, ROWS, 128), jnp.float32),
            pltpu.SemaphoreType.DMA((len(operands),)),
            pltpu.SemaphoreType.DMA((2, groups)),
            pltpu.SemaphoreType.DMA((2, groups)),
        ],
        compiler_params=pltpu.CompilerParams(collective_id=0, has_side_effects=True),
    )(*operands)
    return jnp.transpose(-rate, (2, 0, 1))


def solution(mesh):
    in_specs = (P(None, None, ("dom", "sub")), P(None, ("dom", "sub")))
    out_specs = P(None, None, ("dom", "sub"))
    return jax.shard_map(shards, mesh=mesh, in_specs=in_specs, out_specs=out_specs, check_vma=False)
```

```python
import jax
import jax.numpy as jnp
import numpy as np
import functools

from jax import lax
from jax.experimental import pallas as pl
from jax.experimental.pallas import tpu as pltpu
from jax.sharding import PartitionSpec as P

ORDER = 4


heat_ratio = 1.4
viscosity = 0.08
prandtl = 0.72
penalty = 0.1


def legendre_table(degree, abscissae):
    values = [abscissae * 0.0 + 1.0, abscissae.copy()]
    slopes = [abscissae * 0.0, abscissae * 0.0 + 1.0]
    for current in range(1, degree):
        values.append(
            ((2 * current + 1) * abscissae * values[current] - current * values[current - 1])
            / (current + 1)
        )
        slopes.append(slopes[current - 1] + (2 * current + 1) * values[current])
    return (values, slopes)


def gauss_nodes(degree):
    abscissae = np.cos(np.pi * (np.arange(degree) + 0.75) / (degree + 0.5))
    for unused in range(60):
        values, slopes = legendre_table(degree, abscissae)
        abscissae = abscissae - values[degree] / slopes[degree]
    return np.sort(abscissae)


def operator_tables(degree):
    abscissae = gauss_nodes(degree)
    differ = abscissae[:, None] - abscissae[None, :]
    padded = differ + np.eye(degree)
    weights = 1.0 / np.prod(padded, axis=1)
    derivative = weights[None, :] / weights[:, None] / padded * (1.0 - np.eye(degree))
    derivative = derivative - np.eye(degree) * np.sum(derivative, axis=1)[:, None]
    basis_left = weights / (-1.0 - abscissae)
    basis_left = basis_left / np.sum(basis_left)
    basis_right = weights / (1.0 - abscissae)
    basis_right = basis_right / np.sum(basis_right)
    values, slopes = legendre_table(degree, abscissae)
    right_slope = 0.5 * (slopes[degree - 1] + slopes[degree])
    mirror_values, mirror_slopes = legendre_table(degree, -abscissae)
    left_slope = -0.5 * (mirror_slopes[degree - 1] + mirror_slopes[degree])
    sol_points = degree**3
    face_points = degree**2
    interp = np.zeros((6 * face_points, sol_points))
    grad_matrix = np.zeros((3 * sol_points, sol_points))
    lift_matrix = np.zeros((3 * sol_points, 6 * face_points))
    div_lift = np.zeros((sol_points, 6 * face_points))
    for sol_index in range(sol_points):
        position = (sol_index // face_points, sol_index // degree % degree, sol_index % degree)
        for direction in range(3):
            others = [position[other_dir] for other_dir in range(3) if other_dir != direction]
            flux_index = others[0] * degree + others[1]
            along_index = position[direction]
            for facing in range(2):
                column = (2 * direction + facing) * face_points + flux_index
                interp[column, sol_index] = (basis_left, basis_right)[facing][along_index]
                correct = (left_slope, right_slope)[facing][along_index]
                lift_matrix[direction * sol_points + sol_index, column] = correct
                div_lift[sol_index, column] = (2 * facing - 1) * correct
            for target in range(degree):
                shifted = list(position)
                shifted[direction] = target
                other_point = (shifted[0] * degree + shifted[1]) * degree + shifted[2]
                grad_matrix[direction * sol_points + sol_index, other_point] = derivative[
                    along_index, target
                ]
    normal_matrix = np.zeros((6 * face_points, 3 * sol_points))
    normals = np.zeros((3, 6))
    for face_id in range(6):
        direction = face_id // 2
        orient = 2 * (face_id % 2) - 1
        rows_here = slice(face_id * face_points, (face_id + 1) * face_points)
        normal_matrix[rows_here, direction * sol_points : (direction + 1) * sol_points] = (
            orient * interp[rows_here]
        )
        normals[direction, face_id] = orient
    div_matrix = np.concatenate(
        [
            grad_matrix[direction * sol_points : (direction + 1) * sol_points]
            for direction in range(3)
        ],
        axis=1,
    )
    tables = (interp, grad_matrix, lift_matrix, normal_matrix, div_matrix, div_lift, normals)
    return tables


FACE_LANES = 32
LANES = 256
ROWS = 8
MESH = pl.DeviceIdType.MESH


def halves(table):
    high = np.asarray(table, dtype=jnp.bfloat16)
    low = np.asarray(table - high.astype(np.float64), dtype=jnp.bfloat16)
    return (high, low)


def kernel_tables():
    interp, grad_matrix, lift_matrix, normal_matrix, div_matrix, div_lift, normals = (
        operator_tables(ORDER + 1)
    )
    side = ORDER + 1
    points, face_points = side**3, side**2
    width = 128
    to_lanes = np.zeros((6 * face_points, LANES))
    for face_id in range(6):
        for point in range(face_points):
            to_lanes[face_id * face_points + point, face_id * FACE_LANES + point] = 1.0
    filled = to_lanes.copy()
    spare = to_lanes.sum(axis=0) == 0.0
    filled[0, spare] = 1.0
    trace = np.zeros((width, LANES))
    trace[:points] = interp.T @ filled
    own_grad = np.zeros((width, 3 * width))
    own_spread = np.zeros((width, 3 * LANES))
    jump_grad = np.zeros((LANES, 3 * width))
    jump_spread = np.zeros((LANES, 3 * LANES))
    div = np.zeros((3 * width, width))
    div_all = div_matrix - div_lift @ normal_matrix
    for direction in range(3):
        rows = slice(direction * points, (direction + 1) * points)
        cols = slice(direction * width, direction * width + points)
        wide = slice(direction * LANES, (direction + 1) * LANES)
        own_grad[:points, cols] = grad_matrix[rows].T
        own_spread[:points, wide] = (interp @ grad_matrix[rows]).T @ to_lanes
        jump_grad[:, cols] = to_lanes.T @ (0.5 * lift_matrix[rows]).T
        jump_spread[:, wide] = to_lanes.T @ (interp @ (0.5 * lift_matrix[rows])).T @ to_lanes
        div[cols, :points] = div_all[:, rows].T
    lift = np.zeros((LANES, width))
    lift[:, :points] = to_lanes.T @ div_lift.T
    result = []
    for table in (trace, own_grad, own_spread):
        result.append(table.astype(np.float32))
    for table in (jump_grad, jump_spread):
        result.append(np.stack(halves(table)))
    for table in (div, lift):
        result.append(table.astype(np.float32))
    result.append(np.stack(halves(lift)))
    weights = np.zeros((8, LANES), np.float32)
    for direction in range(3):
        for face_id in range(6):
            start = face_id * FACE_LANES
            weights[direction, start : start + FACE_LANES] = normals[direction, face_id]
    return result + [weights]


def split(value):
    high = value.astype(jnp.bfloat16)
    low = (value - high.astype(jnp.float32)).astype(jnp.bfloat16)
    return (high, low)


def thirds(value):
    high, low = split(value)
    rest = value - high.astype(jnp.float32) - low.astype(jnp.float32)
    return (high, low, rest.astype(jnp.bfloat16))


def mxu(left, right):
    return jnp.dot(left, right, preferred_element_type=jnp.float32)


def table_dot(parts, high, low):
    return mxu(parts[0], high) + mxu(parts[1], high) + mxu(parts[0], low)


def full_dot(left, right):
    return jnp.dot(
        left, right, precision=lax.Precision.HIGHEST, preferred_element_type=jnp.float32
    )


def pick_dot(picks, parts):
    return sum(mxu(picks, part) for part in parts)


def faces_first(blocks, lane, elements):
    per_face = []
    for face_id in range(6):
        tile, inner = divmod(face_id * FACE_LANES, 128)
        total = jnp.zeros((elements, 128), jnp.float32)
        for field_id, block in enumerate(blocks):
            if block is None:
                continue
            shift = (25 * field_id - inner) % 128
            piece = block[:, tile * 128 : tile * 128 + 128]
            if shift:
                piece = pltpu.roll(piece, shift, 1)
            mine = (lane >= 25 * field_id) & (lane < 25 * field_id + 25)
            total = jnp.where(mine, piece, total)
        per_face.append(total)
    return jnp.concatenate(per_face, axis=0)


def fields_first(rows, lane, elements, field_ids, base):
    result = []
    for field_id in field_ids:
        tiles = []
        for tile in range(2):
            total = base[field_id][:, tile * 128 : tile * 128 + 128]
            for face_id in range(tile * 4, min(6, tile * 4 + 4)):
                inner = face_id * FACE_LANES - tile * 128
                shift = (inner - 25 * field_id) % 128
                piece = rows[face_id * elements : (face_id + 1) * elements]
                if shift:
                    piece = pltpu.roll(piece, shift, 1)
                mine = (lane >= inner) & (lane < inner + 25)
                total = jnp.where(mine, piece, total)
            tiles.append(total)
        result.append(jnp.concatenate(tiles, axis=1))
    return result


def divided(value, count):
    return jnp.floor((value + 0.5) * (1.0 / count))


def state_of(fields):
    inverse = 1.0 / fields[0]
    velocity = [fields[1 + b] * inverse for b in range(3)]
    kinetic = 0.5 * (fields[1] * velocity[0] + fields[2] * velocity[1] + fields[3] * velocity[2])
    pressure = (heat_ratio - 1.0) * (fields[4] - kinetic)
    return (inverse, velocity, pressure)


def normal_inviscid(fields, velocity, pressure, normal):
    speed = sum(normal[b] * velocity[b] for b in range(3))
    momentum = sum(normal[b] * fields[1 + b] for b in range(3))
    flux = [momentum]
    for b in range(3):
        flux.append(fields[1 + b] * speed + pressure * normal[b])
    flux.append((fields[4] + pressure) * speed)
    return (flux, speed)


def slopes_of(fields, inverse, velocity, grads):
    slope = [
        [(grads[a][1 + b] - velocity[b] * grads[a][0]) * inverse for a in range(3)]
        for b in range(3)
    ]
    specific = fields[4] * inverse
    energy = []
    for a in range(3):
        value = (grads[a][4] - specific * grads[a][0]) * inverse
        energy.append(value - sum(velocity[b] * slope[b][a] for b in range(3)))
    return (slope, energy)


def body(shape, *refs):
    elements, capacity, sub_count, dom_count = shape
    far, out_ref, held = refs[:11], refs[11], refs[12:23]
    padded, outbox, inbox, load_sem, send_sem, recv_sem = refs[23:]
    sol_ref, link_ref, trace, own_grad_t, own_spread_t, jump_grad, jump_spread, div, lift = held[:9]
    lift_pair, weights_ref = held[9:]
    my_dom, my_sub = lax.axis_index("dom"), lax.axis_index("sub")
    home = 2 * sub_count
    groups = 5 * sub_count
    partners = []
    for offset in range(-2, 3):
        for across in range(sub_count):
            if offset == 0 and across == 0:
                continue
            there = (
                lax.rem(my_dom + offset + dom_count, dom_count),
                lax.rem(my_sub + across, sub_count),
            )
            group = (offset + 2) * sub_count + across
            mirror = (2 - offset) * sub_count + (-across) % sub_count
            partners.append((group, mirror, there))
    barrier = pltpu.get_barrier_semaphore()
    for _, _, there in partners:
        pl.semaphore_signal(barrier, inc=1, device_id=there, device_id_type=MESH)

    def ship(turn):
        copies = []
        for group, mirror, there in partners:
            copies.append(
                pltpu.make_async_remote_copy(
                    src_ref=outbox.at[turn, group],
                    dst_ref=inbox.at[turn, mirror],
                    send_sem=send_sem.at[turn, group],
                    recv_sem=recv_sem.at[turn, mirror],
                    device_id=there,
                    device_id_type=MESH,
                )
            )
            copies[-1].start()
        return copies

    loads = [
        pltpu.make_async_copy(far[i], held[i], load_sem.at[i])
        for i in range(11)
    ]
    for i in (0, 1, 2, 4, 3, 10, 6, 5, 7, 8, 9):
        loads[i].start()

    def loaded(*which):
        for i in which:
            loads[i].wait()

    faces = 6 * elements
    slots = groups * ROWS
    points = sol_ref.shape[2]
    lane = lax.broadcasted_iota(jnp.int32, (elements, 128), 1)

    loaded(0, 2)
    for k in range(5):
        here = sol_ref[k]
        padded[k * elements : (k + 1) * elements, :points] = here
        padded[k * elements : (k + 1) * elements, points:] = here[:, : 128 - points]
    state = padded[...]
    own = full_dot(state, trace[...])

    def by_field(values, start=0, width=LANES):
        return [
            values[k * elements : (k + 1) * elements, start : start + width] for k in range(5)
        ]

    own_fields = by_field(own)
    own_rows = faces_first(own_fields, lane, elements)
    own_parts = thirds(own_rows)

    loaded(1)
    link = link_ref[...].astype(jnp.float32)
    elem = divided(link, 6)
    side = link - 6.0 * elem
    device = divided(elem, elements)
    key = side * elements + (elem - device * elements)
    dom = divided(device, sub_count)
    sub = device - dom * sub_count
    ahead = dom - my_dom.astype(jnp.float32) + 2.0
    ahead = jnp.where(ahead < 0.0, ahead + dom_count, ahead)
    ahead = jnp.where(ahead >= dom_count, ahead - dom_count, ahead)
    across = sub - my_sub.astype(jnp.float32)
    across = jnp.where(across < 0.0, across + sub_count, across)
    group = ahead * sub_count + across

    def as_row(value):
        return jnp.concatenate([value[f : f + 1] for f in range(6)], axis=1)

    group_row = as_row(group)
    key_row = as_row(key)
    both = jnp.concatenate([group_row, key_row] + [group_row] * 6, axis=0).T
    group_col = both[:, 0:1]
    key_col = both[:, 1:2]
    down = lax.broadcasted_iota(jnp.int32, (faces, faces), 0)
    along = lax.broadcasted_iota(jnp.int32, (faces, faces), 1)
    same = group_col == group_row
    send_rank = jnp.sum(jnp.where(same & (down < along), 1.0, 0.0), axis=0, keepdims=True)
    send_slot = jnp.where(group_row == home, -1.0, group_row * ROWS + send_rank)
    slot_down = lax.broadcasted_iota(jnp.int32, (slots, faces), 0).astype(jnp.float32)
    send_pick = jnp.where(send_slot == slot_down, 1.0, 0.0).astype(jnp.bfloat16)

    outbox[0] = pick_dot(send_pick, own_parts).reshape(groups, ROWS, 128)
    pl.semaphore_wait(barrier, len(partners))
    first = ship(0)

    recv_rank = jnp.sum(jnp.where(same & (key_row < key_col), 1.0, 0.0), axis=1, keepdims=True)
    recv_slot = jnp.where(group_col == home, -1.0, group_col * ROWS + recv_rank)
    slot_along = lax.broadcasted_iota(jnp.int32, (faces, slots), 1).astype(jnp.float32)
    recv_pick = jnp.where(recv_slot == slot_along, 1.0, 0.0).astype(jnp.bfloat16)
    near_key = jnp.where(group_col == home, key_col, -1.0)
    near_pick = jnp.where(near_key == along.astype(jnp.float32), 1.0, 0.0).astype(jnp.bfloat16)

    near_rows = pick_dot(near_pick, own_parts)
    loaded(4, 3, 10)
    own_spread = full_dot(state, own_spread_t[...])
    own_grad = full_dot(state, own_grad_t[...])
    normal = [weights_ref[a : a + 1] for a in range(3)]
    inverse, velocity, pressure = state_of(own_fields)
    own_flux, own_speed = normal_inviscid(own_fields, velocity, pressure, normal)
    own_wave = jnp.abs(own_speed) + jnp.sqrt(heat_ratio * pressure * inverse)

    loaded(6)
    inbox[0, home] = jnp.zeros((ROWS, 128), jnp.float32)
    inbox[1, home] = jnp.zeros((ROWS, 128), jnp.float32)
    for copy in first:
        copy.wait_recv()
    arrived = thirds(inbox[0].reshape(slots, 128))
    other_rows = near_rows + pick_dot(recv_pick, arrived)
    other_fields = fields_first(other_rows, lane, elements, range(5), own_fields)
    jump = jnp.concatenate([other_fields[k] - own_fields[k] for k in range(5)], axis=0)
    jump_parts = split(jump)
    spread = own_spread + table_dot(jump_parts, jump_spread[0], jump_spread[1])
    grads = [by_field(spread, a * LANES) for a in range(3)]

    slope, energy = slopes_of(own_fields, inverse, velocity, grads)
    divergence = slope[0][0] + slope[1][1] + slope[2][2]
    own_visc = [None]
    for b in range(3):
        stress = sum(normal[a] * (slope[b][a] + slope[a][b]) for a in range(3))
        own_visc.append(viscosity * stress - (2.0 / 3.0 * viscosity) * normal[b] * divergence)
    heat = sum(normal[a] * energy[a] for a in range(3))
    own_visc.append(
        sum(velocity[b] * own_visc[1 + b] for b in range(3))
        + (viscosity * heat_ratio / prandtl) * heat
    )
    visc_rows = faces_first(own_visc, lane, elements)
    visc_parts = split(visc_rows)
    outbox[1] = pick_dot(send_pick, visc_parts).reshape(groups, ROWS, 128)
    second = ship(1)

    loaded(5, 7, 8, 9)
    near_visc = pick_dot(near_pick, visc_parts)
    grad = own_grad + table_dot(jump_parts, jump_grad[0], jump_grad[1])
    grads = [by_field(grad, a * 128, 128) for a in range(3)]
    fields = by_field(state, 0, 128)
    inner_inverse, inner_velocity, inner_pressure = state_of(fields)
    slope, energy = slopes_of(fields, inner_inverse, inner_velocity, grads)
    divergence = (2.0 / 3.0 * viscosity) * (slope[0][0] + slope[1][1] + slope[2][2])
    total = None
    for a in range(3):
        stress = []
        for b in range(3):
            if a == b:
                stress.append((2.0 * viscosity) * slope[a][a] - divergence)
            else:
                stress.append(viscosity * (slope[b][a] + slope[a][b]))
        flux = [fields[1 + a]]
        for b in range(3):
            member = fields[1 + b] * inner_velocity[a] - stress[b]
            flux.append(member + inner_pressure if a == b else member)
        flux.append(
            (fields[4] + inner_pressure) * inner_velocity[a]
            - sum(inner_velocity[b] * stress[b] for b in range(3))
            - (viscosity * heat_ratio / prandtl) * energy[a]
        )
        rows = slice(a * 128, (a + 1) * 128)
        part = full_dot(jnp.concatenate(flux, axis=0), div[rows])
        total = part if total is None else total + part

    other_inverse, other_velocity, other_pressure = state_of(other_fields)
    other_flux, other_speed = normal_inviscid(
        other_fields, other_velocity, other_pressure, normal
    )
    other_wave = jnp.abs(other_speed) + jnp.sqrt(heat_ratio * other_pressure * other_inverse)
    factor = 0.5 * jnp.maximum(own_wave, other_wave) + penalty
    common = []
    for k in range(5):
        member = 0.5 * (own_flux[k] + other_flux[k]) + factor * (own_fields[k] - other_fields[k])
        common.append(member if k == 0 else member - 0.5 * own_visc[k])
    total = total + full_dot(jnp.concatenate(common, axis=0), lift[...])

    for copy in second:
        copy.wait_recv()
    arrived = split(0.5 * inbox[1].reshape(slots, 128))
    other_rows = 0.5 * near_visc + pick_dot(recv_pick, arrived)
    zeros = [jnp.zeros((elements, LANES), jnp.float32)] * 5
    other_visc = fields_first(other_rows, lane, elements, range(1, 5), zeros)
    lifted = table_dot(split(jnp.concatenate(other_visc, axis=0)), lift_pair[0], lift_pair[1])
    out_ref[0] = total[:elements, :points]
    for k in range(1, 5):
        rows = slice(k * elements, (k + 1) * elements)
        near = slice((k - 1) * elements, k * elements)
        out_ref[k] = total[rows, :points] + lifted[near, :points]
    for copy in first + second:
        copy.wait_send()


def shards(solution, face_link):
    points, fields, elements = solution.shape
    sub_count = lax.axis_size("sub")
    dom_count = lax.axis_size("dom")
    capacity = max(3, elements * 3 // 16)
    assert capacity <= ROWS
    groups = 5 * sub_count
    tables = [jnp.asarray(table) for table in kernel_tables()]
    vmem = pl.BlockSpec(memory_space=pltpu.VMEM)
    operands = [jnp.transpose(solution, (1, 2, 0)), face_link] + tables
    held = [pltpu.VMEM(operand.shape, operand.dtype) for operand in operands]
    rate = pl.pallas_call(
        functools.partial(body, (elements, capacity, sub_count, dom_count)),
        out_shape=pltpu.VMEM((fields, elements, points), jnp.float32),
        in_specs=[pl.BlockSpec(memory_space=pltpu.HBM)] * len(operands),
        out_specs=vmem,
        scratch_shapes=held + [
            pltpu.VMEM((fields * elements, 128), jnp.float32),
            pltpu.VMEM((2, groups, ROWS, 128), jnp.float32),
            pltpu.VMEM((2, groups, ROWS, 128), jnp.float32),
            pltpu.SemaphoreType.DMA((len(operands),)),
            pltpu.SemaphoreType.DMA((2, groups)),
            pltpu.SemaphoreType.DMA((2, groups)),
        ],
        compiler_params=pltpu.CompilerParams(collective_id=0, has_side_effects=True),
    )(*operands)
    return jnp.transpose(-rate, (2, 0, 1))


def solution(mesh):
    in_specs = (P(None, None, ("dom", "sub")), P(None, ("dom", "sub")))
    out_specs = P(None, None, ("dom", "sub"))
    return jax.shard_map(shards, mesh=mesh, in_specs=in_specs, out_specs=out_specs, check_vma=False)
```
